128 devices in a mesh: row: 32 (over x, y, core), col: 4 (over z).
Axes of the slice: x: 4, y: 4, z: 4, core: 2. Of those that a mesh axis runs over, the one named last changes fastest.
Arguments:
- eigvecs: float32 [8192, 4096], P('row', 'col'), may hold values from -6 to 6
- reflectors: float32 [32, 32, 64, 192], P('row'), may hold values from -0.5 to 1.5, as said below
- factors: float32 [32, 32, 64, 64], P('row'), may hold values from -3 to 3, as said below
- first_block: int32 [32], replicated, may hold values from 0 to 31
- live_count: int32 [4], P('col'), may hold values from 128 to 768
Outputs:
- vectors: float32 [8192, 4096], P('row', 'col')
The draws below stay inside these ranges and needn't reach their ends.
Inputs may be any that keep to these rules, and one draw needn't show every extreme that they name: reflectors[w, g, j, 0] lies in 1 to 1.5; the other entries are small. factors[w, g] is upper triangular, and I - V_wg factors[w, g] V_wg^T equals the product over j = 0 .. 63 in order of I - 2 v_j v_j^T / (v_j^T v_j), v_j the columns of V_wg.
All inputs are finite; a program needn't handle non-finite values.
Results may differ from the reference program's by a relative error of at most 0.0003.
Values sent between devices are 32-bit elements; how exact they have to be, the bound alone decides.
A program may use at most 64 MiB of HBM per device.

```python
import jax
import jax.numpy as jnp
from jax import lax

B = 192
NB = 64
CT = 1024
N = 8192
W = 32
NBT = 32
KC = 4096
N_COL = 4


def expand_draw(compact):
    block_width, band_width = compact.shape[-2:]
    block_rows = block_width + band_width
    padded = jnp.pad(compact, ((0, 0), (0, 0), (0, block_rows + 1 - band_width)))
    flattened = padded.reshape(compact.shape[0], block_width * (block_rows + 1))[:, :block_width * block_rows]
    return jnp.swapaxes(flattened.reshape(compact.shape[0], block_width, block_rows), -1, -2)


def reflector_pair(key):
    base = jax.random.fold_in(key, 7)
    shape = (W, NBT, NB, B)
    values = jnp.clip(0.1 * jax.random.normal(base, shape, jnp.float32), -0.5, 0.5)
    first_entry = jnp.arange(B) == 0
    values = jnp.where(first_entry, jnp.abs(values), values)
    leading = first_entry.astype(jnp.float32)
    compact = values + leading

    def window_factors(window_compact):
        expanded_factor = expand_draw(window_compact)
        gram = jnp.einsum('glr,gls->grs', expanded_factor, expanded_factor, precision=lax.Precision.HIGHEST)
        diagonal = jnp.diagonal(gram, axis1=1, axis2=2)
        upper = jnp.triu(gram, 1) + jax.vmap(jnp.diag)(0.5 * diagonal)
        identity = jnp.broadcast_to(jnp.eye(NB, dtype=jnp.float32), upper.shape)
        return jax.scipy.linalg.solve_triangular(upper, identity, lower=False)
    factors = lax.map(window_factors, compact)
    return (compact, factors)


def draw_reflectors(key, part):
    return reflector_pair(key)[0]


def draw_factors(key, part):
    return reflector_pair(key)[1]


def touch_ends(array, key, low, largest):
    shape = array.shape
    place = [jax.random.randint(jax.random.fold_in(key, axis), (), 0, shape[axis]) for axis in range(len(shape))]
    array = array.at[tuple(place)].set(low)
    longest = shape.index(max(shape))
    place[longest] = (place[longest] + 1) % shape[longest]
    return array.at[tuple(place)].set(largest)


def shard_levels(stream_key, shape, shards, smallest, largest):
    gain, own = 1.0, jax.random.fold_in(stream_key, 6)
    for axis_at, blocks in shards:
        steps = jnp.exp(jax.random.uniform(jax.random.fold_in(own, axis_at), (blocks,), jnp.float32, smallest / len(shards), largest / len(shards)))
        gain = gain * jnp.repeat(steps, shape[axis_at] // blocks).reshape([-1 if axis == axis_at else 1 for axis in range(len(shape))])
    return gain


def centred(key, extent, deviation, most, cuts=(), kind=jnp.bfloat16):
    drawn = jax.random.normal(key, extent, jnp.float32) * deviation
    if len(cuts) > 0:
        drawn = shard_levels(key, extent, cuts, -0.22, 0.18) * drawn
    return jnp.clip(drawn, min=-most, max=most).astype(kind)


def setup_inputs(seed: int = 0) -> dict:
    streams_of = jax.random.split(jax.random.key(seed), 6)
    eigvecs = centred(streams_of[0], (N, KC), 1.0, 6.0, ((0, 32), (1, 4)), jnp.float32)
    reflectors = draw_reflectors(jax.random.fold_in(streams_of[5], 71), 0)
    factors = draw_factors(jax.random.fold_in(streams_of[5], 71), 0)
    first_block = touch_ends(jax.random.randint(streams_of[3], (W,), 0, NBT), jax.random.fold_in(streams_of[3], 1), 0, NBT - 1).astype(jnp.int32)
    live_count = touch_ends(jax.random.randint(streams_of[4], (N_COL,), CT // 8, 3 * CT // 4 + 1), jax.random.fold_in(streams_of[4], 1), CT // 8, (3 * CT // 4 + 1) - 1).astype(jnp.int32)
    return dict(eigvecs=eigvecs, reflectors=reflectors, factors=factors, first_block=first_block, live_count=live_count)


highest_precision = lax.Precision.HIGHEST

def expand(compact):
    leading = compact.shape[:-2]
    block_width, band_width = compact.shape[-2:]
    block_rows = block_width + band_width
    padded = jnp.pad(compact, [(0, 0)] * len(leading) + [(0, 0), (0, block_rows + 1 - band_width)])
    flattened = padded.reshape(leading + (block_width * (block_rows + 1),))[..., :block_width * block_rows]
    return jnp.swapaxes(flattened.reshape(leading + (block_width, block_rows)), -1, -2)

def apply_blocks(eigenvector_blocks, compact, factor):
    expanded_factor = expand(compact)
    correlation_matrix = jnp.einsum('kpx,kpi->kxi', expanded_factor, eigenvector_blocks, precision=highest_precision)
    correlation_matrix = jnp.einsum('grs,gsc->grc', factor, correlation_matrix, precision=highest_precision)
    return eigenvector_blocks - jnp.einsum('nfu,nuo->nfo', expanded_factor, correlation_matrix, precision=highest_precision)

def reference(eigvecs, reflectors, factors, first_block, live_count):
    block_rows = NB + B
    half_block = block_rows // 2
    vectors = eigvecs
    block_index = jnp.arange(NBT, dtype=jnp.int32)
    for window in range(W):
        active_window = (block_index >= first_block[window])[:, None, None]
        if window % 2 == 0:
            blocks = vectors.reshape(NBT, block_rows, KC)
            updated = apply_blocks(blocks, reflectors[window], factors[window])
            vectors = jnp.where(active_window, updated, blocks).reshape(N, KC)
        else:
            blocks = vectors[half_block:N - half_block].reshape(NBT - 1, block_rows, KC)
            updated = apply_blocks(blocks, reflectors[window, :NBT - 1], factors[window, :NBT - 1])
            updated = jnp.where(active_window[:NBT - 1], updated, blocks).reshape(N - block_rows, KC)
            vectors = jnp.concatenate([vectors[:half_block], updated, vectors[N - half_block:]], axis=0)
    slot_index = jnp.arange(KC, dtype=jnp.int32) % CT
    column_group = jnp.arange(KC, dtype=jnp.int32) // CT
    kept_mask = slot_index < live_count[column_group]
    return jnp.where(kept_mask[None, :], vectors, jnp.zeros_like(vectors))
```

```python
import functools

import jax
import jax.numpy as jnp
from jax import lax
from jax.experimental import pallas as pl
from jax.experimental.pallas import tpu as pltpu
from jax.sharding import PartitionSpec as P

HIGHEST = lax.Precision.HIGHEST
MAX_LIVE = 768
CHUNK = 256
AHEAD = 3
F32 = jnp.float32
BF16 = jnp.bfloat16


def split(x):
    hi = x.astype(BF16)
    lo = (x - hi.astype(F32)).astype(BF16)
    return hi, lo


def dot(a, b):
    return jnp.dot(a, b, preferred_element_type=F32)


def dot_full(a, b, dims=(((1,), (0,)), ((), ()))):
    return lax.dot_general(a, b, dims, precision=HIGHEST, preferred_element_type=F32)


TN = (((0,), (0,)), ((), ()))


def kernel(
    n_row,
    eig_ref,
    refl_ref,
    out_ref,
    y_ref,
    g_ref,
    cs_ref,
    cr_ref,
    fw_ref,
    rh_ref,
    rl_ref,
    sh_ref,
    sl_ref,
    hs_ref,
    hl_ref,
    w_ref,
    ws_ref,
    wl_ref,
    send_sem,
    recv_sem,
    fsend_sem,
    frecv_sem,
):
    d = lax.axis_index("row")
    has_up = d > 0
    has_dn = d < n_row - 1
    windows, nb, block_rows = refl_ref.shape
    rounds = windows // 2
    half = block_rows // 2
    band = block_rows - nb
    n_chunks = y_ref.shape[0]

    def link(way, p, c):
        src = cs_ref.at[p, c, pl.ds(way * nb, nb)]
        dst = cr_ref.at[p, c, pl.ds((1 - way) * nb, nb)]
        return pltpu.make_async_remote_copy(
            src_ref=src,
            dst_ref=dst,
            send_sem=send_sem.at[way, p, c],
            recv_sem=recv_sem.at[way, p, c],
            device_id={"row": d + 2 * way - 1},
            device_id_type=pl.DeviceIdType.MESH,
        )

    def forward(r):
        return pltpu.make_async_remote_copy(
            src_ref=refl_ref.at[2 * r + 1],
            dst_ref=fw_ref.at[r],
            send_sem=fsend_sem.at[r],
            recv_sem=frecv_sem.at[r],
            device_id={"row": d + 1},
            device_id_type=pl.DeviceIdType.MESH,
        )

    barrier = pltpu.get_barrier_semaphore()

    @pl.when(has_up)
    def _():
        pl.semaphore_signal(
            barrier, inc=1, device_id={"row": d - 1}, device_id_type=pl.DeviceIdType.MESH
        )

    @pl.when(has_dn)
    def _():
        pl.semaphore_signal(
            barrier, inc=1, device_id={"row": d + 1}, device_id_type=pl.DeviceIdType.MESH
        )

    inside = has_up & has_dn

    @pl.when(inside)
    def _():
        pl.semaphore_wait(barrier, 2)

    @pl.when(jnp.logical_not(inside))
    def _():
        pl.semaphore_wait(barrier, 1)

    @pl.when(has_dn)
    def _():
        for r in range(min(AHEAD, rounds)):
            forward(r).start()

    @pl.when(jnp.logical_not(has_up))
    def _():
        fw_ref[...] = jnp.zeros_like(fw_ref)
        for p in range(2):
            for c in range(n_chunks):
                cr_ref[p, c, pl.ds(0, nb)] = jnp.zeros((nb, CHUNK), F32)

    @pl.when(jnp.logical_not(has_dn))
    def _():
        for p in range(2):
            for c in range(n_chunks):
                cr_ref[p, c, pl.ds(nb, nb)] = jnp.zeros((nb, CHUNK), F32)

    def expanded(block):
        lane = lax.broadcasted_iota(jnp.int32, (nb, block_rows), 1)
        return pltpu.roll(jnp.where(lane < band, block, 0.0), 0, 1, stride=1, stride_axis=0)

    lane_h = lax.broadcasted_iota(jnp.int32, (nb, half), 1)

    def prepare_even(r):
        block = refl_ref[2 * r]
        vt = expanded(block)
        factor = jnp.where(lane_h >= half - nb, block[:, half:], 0.0)
        u = dot_full(factor, jnp.concatenate([vt, vt], axis=0))
        op = dot_full(vt, u, TN)
        hi, lo = split(op)
        rh_ref[...] = hi
        rl_ref[...] = lo
        return op

    def prepare_odd(r, op):
        q = lax.rem(r, 2)
        own = refl_ref[2 * r + 1]
        other = fw_ref[r]
        none = jnp.zeros((nb, half), F32)
        proj = jnp.concatenate(
            [
                jnp.concatenate([expanded(other)[:, half:], none], axis=1),
                jnp.concatenate([none, expanded(own)[:, :half]], axis=1),
            ],
            axis=0,
        )
        both = jnp.concatenate(
            [
                jnp.where(lane_h < nb, pltpu.roll(other[:, half:], nb, 1), 0.0),
                jnp.where(lane_h >= half - nb, own[:, half:], 0.0),
            ],
            axis=0,
        )
        w = dot_full(proj, both, TN)
        w_ref[q] = w
        whi, wlo = split(w)
        ws_ref[q] = jnp.concatenate([whi, whi], axis=1)
        wl_ref[q] = wlo
        s = proj - dot_full(proj, op)
        shi, slo = split(s)
        sh_ref[...] = shi
        sl_ref[...] = slo
        return s

    def prepare_link(r, s):
        h = dot_full(s, w_ref[1 - lax.rem(r, 2)])
        hhi, hlo = split(h)
        hs_ref[...] = jnp.concatenate([hhi, hhi], axis=1)
        hl_ref[...] = hlo

    def arrive(r):
        @pl.when(has_up)
        def _():
            forward(r).wait_recv()

    def launch(p, c):
        @pl.when(has_up)
        def _():
            link(0, p, c).start()

        @pl.when(has_dn)
        def _():
            link(1, p, c).start()

    def land(p, c):
        @pl.when(has_up)
        def _():
            link(0, p, c).wait_send()
            link(1, p, c).wait_recv()

        @pl.when(has_dn)
        def _():
            link(1, p, c).wait_send()
            link(0, p, c).wait_recv()

    def project(y):
        yh, yl = split(y)
        return dot(sh_ref[...], yh) + (dot(sl_ref[...], yh) + dot(sh_ref[...], yl))

    def reflect(z):
        zh, zl = split(z)
        return z - (dot(rh_ref[...], zh) + (dot(rl_ref[...], zh) + dot(rh_ref[...], zl)))

    def columns(c):
        return pl.ds(c * CHUNK, CHUNK)

    op = prepare_even(0)
    arrive(0)
    prepare_odd(0, op)
    for c in range(n_chunks):
        cs_ref[0, c] = project(eig_ref[:, columns(c)])
        launch(0, c)
    for c in range(n_chunks):
        y_ref[c] = reflect(eig_ref[:, columns(c)])

    def next_round(r):
        op = prepare_even(r)
        arrive(r)
        s = prepare_odd(r, op)
        prepare_link(r, s)
        for c in range(n_chunks):
            g_ref[c] = project(y_ref[c])

    next_round(1)

    def step(r, carry):
        p = lax.rem(r, 2)

        @pl.when(has_dn & (r + AHEAD < rounds))
        def _():
            forward(r + AHEAD).start()

        for c in range(n_chunks):
            land(p, c)
            total = cs_ref[p, c] + cr_ref[p, c]
            thi, tlo = split(total)
            stacked = jnp.concatenate([thi, tlo], axis=0)
            cs_ref[1 - p, c] = g_ref[c] - (dot(hs_ref[...], stacked) + dot(hl_ref[...], thi))
            launch(1 - p, c)
            z = y_ref[c] - (dot(ws_ref[p], stacked) + dot(wl_ref[p], thi))
            y_ref[c] = reflect(z)

        @pl.when(r + 2 < rounds)
        def _():
            next_round(r + 2)

        return carry

    lax.fori_loop(0, rounds - 1, step, 0)

    p = (rounds - 1) % 2
    for c in range(n_chunks):
        land(p, c)
        total = cs_ref[p, c] + cr_ref[p, c]
        thi, tlo = split(total)
        stacked = jnp.concatenate([thi, tlo], axis=0)
        out_ref[:, columns(c)] = y_ref[c] - (dot(ws_ref[p], stacked) + dot(wl_ref[p], thi))

    @pl.when(has_dn)
    def _():
        def done(r, carry):
            forward(r).wait_send()
            return carry

        lax.fori_loop(0, rounds, done, 0)


def sweep(eigvecs, packed, n_row):
    rows = eigvecs.shape[0]
    windows, nb, block_rows = packed.shape
    rounds = windows // 2
    n_chunks = MAX_LIVE // CHUNK
    vmem = pltpu.VMEM
    return pl.pallas_call(
        functools.partial(kernel, n_row),
        out_shape=jax.ShapeDtypeStruct((rows, MAX_LIVE), F32),
        grid=(1,),
        in_specs=[
            pl.BlockSpec((rows, MAX_LIVE), lambda i: (0, 0)),
            pl.BlockSpec((windows, nb, block_rows), lambda i: (0, 0, 0)),
        ],
        out_specs=pl.BlockSpec((rows, MAX_LIVE), lambda i: (0, 0)),
        scratch_shapes=[
            vmem((n_chunks, rows, CHUNK), F32),
            vmem((n_chunks, 2 * nb, CHUNK), F32),
            vmem((2, n_chunks, 2 * nb, CHUNK), F32),
            vmem((2, n_chunks, 2 * nb, CHUNK), F32),
            vmem((rounds, nb, block_rows), F32),
            vmem((rows, rows), BF16),
            vmem((rows, rows), BF16),
            vmem((2 * nb, rows), BF16),
            vmem((2 * nb, rows), BF16),
            vmem((2 * nb, 4 * nb), BF16),
            vmem((2 * nb, 2 * nb), BF16),
            vmem((2, rows, 2 * nb), F32),
            vmem((2, rows, 4 * nb), BF16),
            vmem((2, rows, 2 * nb), BF16),
            pltpu.SemaphoreType.DMA((2, 2, n_chunks)),
            pltpu.SemaphoreType.DMA((2, 2, n_chunks)),
            pltpu.SemaphoreType.DMA((rounds,)),
            pltpu.SemaphoreType.DMA((rounds,)),
        ],
        compiler_params=pltpu.CompilerParams(
            collective_id=0, has_side_effects=True, vmem_limit_bytes=48 * 2**20
        ),
        name="sweep",
    )(eigvecs, packed)


def body(eigvecs, reflectors, factors, first_block, live_count):
    n_row = lax.axis_size("row")
    position = lax.axis_index("row")
    share, blocks = reflectors.shape[:2]
    window = position * share + jnp.arange(share, dtype=jnp.int32)
    block = jnp.arange(blocks, dtype=jnp.int32)
    applied = block[None, :] >= first_block[window][:, None]
    applied &= (window[:, None] % 2 == 0) | (block[None, :] < blocks - 1)
    factors = jnp.where(applied[:, :, None, None], factors, 0.0)
    packed = jnp.concatenate([reflectors, factors], axis=3)
    packed = lax.all_to_all(packed, "row", split_axis=1, concat_axis=0, tiled=True)
    packed = packed.reshape((packed.shape[0],) + packed.shape[2:])
    vectors = sweep(eigvecs, packed, n_row)
    col_count = eigvecs.shape[1]
    vectors = jnp.pad(vectors, ((0, 0), (0, col_count - MAX_LIVE)))
    kept_mask = jnp.arange(col_count, dtype=jnp.int32) < live_count[0]
    return jnp.where(kept_mask[None, :], vectors, 0.0)


def solution(mesh):
    placed = (
        P("row", "col"),
        P("row", None, None, None),
        P("row", None, None, None),
        P(),
        P("col"),
    )
    return jax.shard_map(
        body, mesh=mesh, in_specs=placed, out_specs=P("row", "col"), check_vma=False
    )
```

```python
import functools

import jax
import jax.numpy as jnp
from jax import lax
from jax.experimental import pallas as pl
from jax.experimental.pallas import tpu as pltpu
from jax.sharding import PartitionSpec as P

MAX_LIVE = 768
CHUNK = 256
AHEAD = 3
LEAD = 12
F32 = jnp.float32
BF16 = jnp.bfloat16
MESH = pl.DeviceIdType.MESH
TN = (((0,), (0,)), ((), ()))


def split(x):
    hi = x.astype(BF16)
    lo = (x - hi.astype(F32)).astype(BF16)
    return hi, lo


def dot(a, b):
    return jnp.dot(a, b, preferred_element_type=F32)


def dot_tn(a, b):
    return lax.dot_general(a, b, TN, preferred_element_type=F32)


def kernel(
    n_row,
    n_col,
    first_ref,
    eig_hbm,
    refl_hbm,
    fact_hbm,
    out_ref,
    e_ref,
    v_ref,
    t_ref,
    pk_ref,
    got_ref,
    fw_ref,
    y_ref,
    g_ref,
    st_ref,
    cs_ref,
    cr_ref,
    rh_ref,
    rl_ref,
    sh_ref,
    sl_ref,
    hs_ref,
    hl_ref,
    ws_ref,
    wl_ref,
    local_sem,
    eig_sem,
    asend_sem,
    rsend_sem,
    arecv_sem,
    send_sem,
    recv_sem,
    fsend_sem,
    frecv_sem,
):
    d = lax.axis_index("row")
    z = lax.axis_index("col")
    has_up = d > 0
    has_dn = d < n_row - 1
    windows, nb, block_rows = got_ref.shape
    band = block_rows - nb
    rounds = windows // 2
    half = block_rows // 2
    n_chunks = y_ref.shape[0]
    n_peers = n_row // n_col
    kin = lax.rem(z - d + n_row * n_col, n_col)

    def peer(j):
        return kin + n_col * j

    barrier = pltpu.get_barrier_semaphore()

    def greet(cond, where):
        @pl.when(cond)
        def _():
            pl.semaphore_signal(barrier, inc=1, device_id=where, device_id_type=MESH)

    for j in range(n_peers):
        greet(peer(j) != d, {"row": peer(j)})
    for o in range(1, n_col):
        pl.semaphore_signal(
            barrier, inc=1, device_id={"col": lax.rem(z + o, n_col)}, device_id_type=MESH
        )
    greet(has_up, {"row": d - 1})
    greet(has_dn, {"row": d + 1})

    def fetch(j):
        t = peer(j) if j < n_peers else d
        return (
            pltpu.make_async_copy(refl_hbm.at[0, t], v_ref.at[j], local_sem.at[0, j]),
            pltpu.make_async_copy(fact_hbm.at[0, t], t_ref.at[j], local_sem.at[1, j]),
        )

    for j in range(n_peers + 1):
        for copy in fetch(j):
            copy.start()
    eig_copy = pltpu.make_async_copy(
        eig_hbm.at[:, pl.ds(0, n_chunks * CHUNK)], e_ref, eig_sem
    )
    eig_copy.start()

    @pl.when(jnp.logical_not(has_up))
    def _():
        fw_ref[...] = jnp.zeros_like(fw_ref)
        for p in range(2):
            for c in range(n_chunks):
                cr_ref[p, c, pl.ds(0, nb)] = jnp.zeros((nb, CHUNK), F32)

    @pl.when(jnp.logical_not(has_dn))
    def _():
        for p in range(2):
            for c in range(n_chunks):
                cr_ref[p, c, pl.ds(nb, nb)] = jnp.zeros((nb, CHUNK), F32)

    for j in range(n_peers + 1):
        for copy in fetch(j):
            copy.wait()
        packed = jnp.concatenate([v_ref[j], t_ref[j]], axis=1)
        if j < n_peers:
            pk_ref[j] = packed
        else:
            got_ref[d] = packed

    ups = (d + n_row - 1) // n_row
    downs = (2 * n_row - 2 - d) // n_row
    others = (lax.rem(2 * d - z + n_row * n_col, n_col) + n_col - 1) // n_col
    pl.semaphore_wait(barrier, n_peers - 1 + others + n_col - 1 + ups + downs)

    def give(j):
        return pltpu.make_async_remote_copy(
            src_ref=pk_ref.at[j],
            dst_ref=got_ref.at[d],
            send_sem=asend_sem.at[j],
            recv_sem=arecv_sem.at[d],
            device_id={"row": peer(j)},
            device_id_type=MESH,
        )

    def relay(j, o):
        w = peer(j)
        return pltpu.make_async_remote_copy(
            src_ref=got_ref.at[w],
            dst_ref=got_ref.at[w],
            send_sem=rsend_sem.at[o - 1, j],
            recv_sem=arecv_sem.at[w],
            device_id={"col": lax.rem(z + o, n_col)},
            device_id_type=MESH,
        )

    def incoming(w):
        return pltpu.make_async_remote_copy(
            src_ref=got_ref.at[w],
            dst_ref=got_ref.at[w],
            send_sem=rsend_sem.at[0, 0],
            recv_sem=arecv_sem.at[w],
            device_id={"col": lax.rem(z + 1, n_col)},
            device_id_type=MESH,
        )

    def pass_on(j, cond=True):
        @pl.when((peer(j) != d) & cond)
        def _():
            incoming(peer(j)).wait_recv()
            for o in range(1, n_col):
                relay(j, o).start()

    def need(w, cond=True):
        @pl.when((w != d) & (lax.rem(w + d, n_col) != z) & cond)
        def _():
            incoming(w).wait_recv()

    def forward(r):
        return pltpu.make_async_remote_copy(
            src_ref=got_ref.at[2 * r + 1],
            dst_ref=fw_ref.at[r],
            send_sem=fsend_sem.at[r],
            recv_sem=frecv_sem.at[r],
            device_id={"row": d + 1},
            device_id_type=MESH,
        )

    def send_on(r, cond=True):
        need(2 * r + 1, cond)

        @pl.when(has_dn & cond)
        def _():
            forward(r).start()

    def arrive(r, cond=True):
        @pl.when(has_up & cond)
        def _():
            forward(r).wait_recv()

    def link(way, p, c):
        return pltpu.make_async_remote_copy(
            src_ref=cs_ref.at[p, c, pl.ds(way * nb, nb)],
            dst_ref=cr_ref.at[p, c, pl.ds((1 - way) * nb, nb)],
            send_sem=send_sem.at[way, p, c],
            recv_sem=recv_sem.at[way, p, c],
            device_id={"row": d + 2 * way - 1},
            device_id_type=MESH,
        )

    def launch(p, c):
        @pl.when(has_up)
        def _():
            link(0, p, c).start()

        @pl.when(has_dn)
        def _():
            link(1, p, c).start()

    def land(p, c):
        @pl.when(has_up)
        def _():
            link(0, p, c).wait_send()
            link(1, p, c).wait_recv()

        @pl.when(has_dn)
        def _():
            link(1, p, c).wait_send()
            link(0, p, c).wait_recv()

    lane = lax.broadcasted_iota(jnp.int32, (nb, block_rows), 1)
    lane_h = lax.broadcasted_iota(jnp.int32, (nb, half), 1)

    def expanded(block):
        return pltpu.roll(jnp.where(lane < band, block, 0.0), 0, 1, stride=1, stride_axis=0)

    def prepare_even(r):
        block = got_ref[2 * r]
        vh, vl = split(expanded(block))
        on = d >= first_ref[2 * r]
        factor = jnp.where((lane_h >= half - nb) & on, block[:, half:], 0.0)
        th = factor.astype(BF16).astype(F32)
        tl = factor - th
        left = jnp.concatenate([th + pltpu.roll(th, nb, 1), pltpu.roll(tl, nb, 1)], axis=1)
        u = dot(left.astype(BF16), jnp.concatenate([vh, vl, vh, vh], axis=0))
        uh, ul = split(u)
        op = dot_tn(
            jnp.concatenate([vh, vh, vl, jnp.zeros_like(vh)], axis=0),
            jnp.concatenate([uh, ul, uh, uh], axis=0),
        )
        hi, lo = split(op)
        rh_ref[...] = hi
        rl_ref[...] = lo
        return hi, lo

    def prepare_odd(r, oh, ol):
        q = lax.rem(r, 2)
        own = got_ref[2 * r + 1]
        other = fw_ref[r]
        first = first_ref[2 * r + 1]
        none = jnp.zeros((nb, half), F32)
        proj = jnp.concatenate(
            [
                jnp.concatenate([expanded(other)[:, half:], none], axis=1),
                jnp.concatenate([none, expanded(own)[:, :half]], axis=1),
            ],
            axis=0,
        )
        both = jnp.concatenate(
            [
                jnp.where(
                    (lane_h < nb) & (d - 1 >= first), pltpu.roll(other[:, half:], nb, 1), 0.0
                ),
                jnp.where((lane_h >= half - nb) & (d >= first) & has_dn, own[:, half:], 0.0),
            ],
            axis=0,
        )
        ph, pm = split(proj)
        bh, bl = split(both)
        w = dot_tn(
            jnp.concatenate([ph, pm], axis=0), jnp.concatenate([bh, bh], axis=0)
        ) + dot_tn(ph, bl)
        wh, wl = split(w)
        ws_ref[q] = jnp.concatenate([wh, wh], axis=1)
        wl_ref[q] = wl
        s = proj - (dot(ph, oh) + (dot(pm, oh) + dot(ph, ol)))
        sh, sl = split(s)
        sh_ref[...] = sh
        sl_ref[...] = sl
        return sh, sl

    def prepare_link(r, sh, sl):
        q = 1 - lax.rem(r, 2)
        wh = ws_ref[q, :, pl.ds(0, half)]
        h = dot(sh, wh) + (dot(sl, wh) + dot(sh, wl_ref[q]))
        hh, hl = split(h)
        hs_ref[...] = jnp.concatenate([hh, hh], axis=1)
        hl_ref[...] = hl

    def project(y):
        yh, yl = split(y)
        return dot(sh_ref[...], yh) + (dot(sl_ref[...], yh) + dot(sh_ref[...], yl))

    def reflect(x):
        xh, xl = split(x)
        return x - (dot(rh_ref[...], xh) + (dot(rl_ref[...], xh) + dot(rh_ref[...], xl)))

    def corrected(p, c):
        return y_ref[c] - (dot(ws_ref[p], st_ref[c]) + dot(wl_ref[p], st_ref[c, pl.ds(0, half)]))

    def total(p, c):
        th, tl = split(cs_ref[p, c] + cr_ref[p, c])
        st_ref[c] = jnp.concatenate([th, tl], axis=0)

    def columns(c):
        return pl.ds(c * CHUNK, CHUNK)

    turn = d // n_col
    for j in range(n_peers):
        k = lax.rem(j + turn, n_peers)

        @pl.when(peer(k) != d)
        def _():
            give(k).start()

    lead = min(LEAD // n_col, n_peers)
    for j in range(lead):
        pass_on(j)

    send_on(0)
    need(0)
    oh, ol = prepare_even(0)
    for r in range(1, min(AHEAD, rounds)):
        send_on(r)
    arrive(0)
    prepare_odd(0, oh, ol)
    eig_copy.wait()
    for c in range(n_chunks):
        cs_ref[0, c] = project(e_ref[:, columns(c)])
        launch(0, c)

    need(2)
    arrive(1)
    for c in range(n_chunks):
        y_ref[c] = reflect(e_ref[:, columns(c)])
    prepare_link(1, *prepare_odd(1, *prepare_even(1)))
    for c in range(n_chunks):
        g_ref[c] = project(y_ref[c])

    def step(r, carry):
        p = lax.rem(r, 2)
        for c in range(n_chunks):
            land(p, c)
            total(p, c)
            cs_ref[1 - p, c] = g_ref[c] - (
                dot(hs_ref[...], st_ref[c]) + dot(hl_ref[...], st_ref[c, pl.ds(0, half)])
            )
            launch(1 - p, c)

        now = (2 * r + LEAD) // n_col
        pass_on(now, ((2 * r + 2 + LEAD) // n_col > now) & (now < n_peers))
        send_on(r + AHEAD, r + AHEAD < rounds)
        need(2 * r + 4, r + 2 < rounds)
        arrive(r + 2, r + 2 < rounds)

        for c in range(n_chunks):
            y_ref[c] = reflect(corrected(p, c))
        after = jnp.minimum(r + 2, rounds - 1)
        prepare_link(after, *prepare_odd(after, *prepare_even(after)))
        for c in range(n_chunks):
            g_ref[c] = project(y_ref[c])
        return carry

    lax.fori_loop(0, rounds - 1, step, 0)

    p = (rounds - 1) % 2
    for c in range(n_chunks):
        land(p, c)
        total(p, c)
        out_ref[:, columns(c)] = corrected(p, c)

    for j in range(n_peers):

        @pl.when(peer(j) != d)
        def _():
            give(j).wait_send()
            for o in range(1, n_col):
                relay(j, o).wait_send()

    @pl.when(has_dn)
    def _():
        def done(r, carry):
            forward(r).wait_send()
            return carry

        lax.fori_loop(0, rounds, done, 0)


def sweep(eigvecs, reflectors, factors, first_block, n_row, n_col):
    rows = eigvecs.shape[0]
    nb, band = reflectors.shape[2:]
    block_rows = nb + band
    windows = n_row * reflectors.shape[0]
    rounds = windows // 2
    n_chunks = MAX_LIVE // CHUNK
    n_peers = n_row // n_col
    vmem = pltpu.VMEM
    dma = pltpu.SemaphoreType.DMA
    return pl.pallas_call(
        functools.partial(kernel, n_row, n_col),
        out_shape=jax.ShapeDtypeStruct((rows, MAX_LIVE), F32),
        in_specs=[
            pl.BlockSpec(memory_space=pltpu.SMEM),
            pl.BlockSpec(memory_space=pl.ANY),
            pl.BlockSpec(memory_space=pl.ANY),
            pl.BlockSpec(memory_space=pl.ANY),
        ],
        out_specs=pl.BlockSpec(memory_space=pltpu.VMEM),
        scratch_shapes=[
            vmem((rows, MAX_LIVE), F32),
            vmem((n_peers + 1, nb, band), F32),
            vmem((n_peers + 1, nb, nb), F32),
            vmem((n_peers, nb, block_rows), F32),
            vmem((windows, nb, block_rows), F32),
            vmem((rounds, nb, block_rows), F32),
            vmem((n_chunks, rows, CHUNK), F32),
            vmem((n_chunks, 2 * nb, CHUNK), F32),
            vmem((n_chunks, 4 * nb, CHUNK), BF16),
            vmem((2, n_chunks, 2 * nb, CHUNK), F32),
            vmem((2, n_chunks, 2 * nb, CHUNK), F32),
            vmem((rows, rows), BF16),
            vmem((rows, rows), BF16),
            vmem((2 * nb, rows), BF16),
            vmem((2 * nb, rows), BF16),
            vmem((2 * nb, 4 * nb), BF16),
            vmem((2 * nb, 2 * nb), BF16),
            vmem((2, rows, 4 * nb), BF16),
            vmem((2, rows, 2 * nb), BF16),
            dma((2, n_peers + 1)),
            dma,
            dma((n_peers,)),
            dma((max(n_col - 1, 1), n_peers)),
            dma((windows,)),
            dma((2, 2, n_chunks)),
            dma((2, 2, n_chunks)),
            dma((rounds,)),
            dma((rounds,)),
        ],
        compiler_params=pltpu.CompilerParams(
            collective_id=0, has_side_effects=True, vmem_limit_bytes=40 * 2**20
        ),
        name="sweep",
    )(first_block, eigvecs, reflectors, factors)


def body(eigvecs, reflectors, factors, first_block, live_count):
    n_row = lax.axis_size("row")
    n_col = lax.axis_size("col")
    vectors = sweep(eigvecs, reflectors, factors, first_block, n_row, n_col)
    col_count = eigvecs.shape[1]
    vectors = jnp.pad(vectors, ((0, 0), (0, col_count - MAX_LIVE)))
    kept_mask = jnp.arange(col_count, dtype=jnp.int32) < live_count[0]
    return jnp.where(kept_mask[None, :], vectors, 0.0)


def solution(mesh):
    placed = (
        P("row", "col"),
        P("row", None, None, None),
        P("row", None, None, None),
        P(),
        P("col"),
    )
    return jax.shard_map(
        body, mesh=mesh, in_specs=placed, out_specs=P("row", "col"), check_vma=False
    )
```

```python
import functools

import jax
import jax.numpy as jnp
from jax import lax
from jax.experimental import pallas as pl
from jax.experimental.pallas import tpu as pltpu
from jax.sharding import PartitionSpec as P

MAX_LIVE = 768
CHUNK = 256
AHEAD = 4
LEAD = 16
FIRST = 8
SLOTS = 4
F32 = jnp.float32
BF16 = jnp.bfloat16
MESH = pl.DeviceIdType.MESH
TN = (((0,), (0,)), ((), ()))


def split(x):
    hi = x.astype(BF16)
    lo = (x - hi.astype(F32)).astype(BF16)
    return hi, lo


def dot(a, b):
    return jnp.dot(a, b, preferred_element_type=F32)


def dot_tn(a, b):
    return lax.dot_general(a, b, TN, preferred_element_type=F32)


def kernel(
    n_row,
    n_col,
    first_ref,
    eig_hbm,
    refl_hbm,
    fact_hbm,
    out_ref,
    e_ref,
    v_ref,
    t_ref,
    pk_ref,
    got_ref,
    fw_ref,
    y_ref,
    g_ref,
    d_ref,
    st_ref,
    cs_ref,
    cr_ref,
    hsend_ref,
    hrecv_ref,
    rh_ref,
    rl_ref,
    sh_ref,
    sl_ref,
    ho_ref,
    hd_ref,
    ws_ref,
    wl_ref,
    local_sem,
    eig_sem,
    asend_sem,
    rsend_sem,
    arecv_sem,
    send_sem,
    recv_sem,
    fsend_sem,
    frecv_sem,
    hsend_sem,
    hrecv_sem,
):
    d = lax.axis_index("row")
    z = lax.axis_index("col")
    windows, nb, block_rows = got_ref.shape
    band = block_rows - nb
    rounds = windows // 2
    half = block_rows // 2
    n_chunks = y_ref.shape[0]
    n_peers = n_row // n_col
    kin = lax.rem(z - d + n_row * n_col, n_col)

    odd = lax.rem(d, 2)
    is_odd = odd == 1
    has_up = d > 0
    has_dn = d < n_row - 1
    has_edge = (has_up & has_dn, None)
    across = (d - 1 + 2 * odd, d + 1 - 2 * odd)

    def only(cond, todo):
        if cond is None:
            todo()
        else:
            pl.when(cond)(todo)

    def peer(j):
        return kin + n_col * j

    barrier = pltpu.get_barrier_semaphore()

    def greet(cond, where):
        @pl.when(cond)
        def _():
            pl.semaphore_signal(barrier, inc=1, device_id=where, device_id_type=MESH)

    for j in range(n_peers):
        greet(peer(j) != d, {"row": peer(j)})
    for o in range(1, n_col):
        pl.semaphore_signal(
            barrier, inc=1, device_id={"col": lax.rem(z + o, n_col)}, device_id_type=MESH
        )
    greet(has_up, {"row": d - 1})
    greet(has_dn, {"row": d + 1})

    def fetch(j):
        t = peer(j) if j < n_peers else d
        return (
            pltpu.make_async_copy(refl_hbm.at[0, t], v_ref.at[j], local_sem.at[0, j]),
            pltpu.make_async_copy(fact_hbm.at[0, t], t_ref.at[j], local_sem.at[1, j]),
        )

    for j in range(n_peers + 1):
        for copy in fetch(j):
            copy.start()
    eig_copy = pltpu.make_async_copy(
        eig_hbm.at[:, pl.ds(0, n_chunks * CHUNK)], e_ref, eig_sem
    )
    eig_copy.start()

    @pl.when(jnp.logical_not(has_up))
    def _():
        fw_ref[...] = jnp.zeros_like(fw_ref)

    @pl.when(jnp.logical_not(has_edge[0]))
    def _():
        for r in range(rounds):
            hrecv_ref[r, 0] = jnp.zeros((nb // 2, half), F32)
        for p in range(SLOTS):
            for c in range(n_chunks):
                cr_ref[p, c, 0] = jnp.zeros((nb, CHUNK), F32)

    for j in range(n_peers + 1):
        for copy in fetch(j):
            copy.wait()
        packed = jnp.concatenate([v_ref[j], t_ref[j]], axis=1)
        if j < n_peers:
            pk_ref[j] = packed
        else:
            got_ref[d] = packed

    ups = (d + n_row - 1) // n_row
    downs = (2 * n_row - 2 - d) // n_row
    others = (lax.rem(2 * d - z + n_row * n_col, n_col) + n_col - 1) // n_col
    pl.semaphore_wait(barrier, n_peers - 1 + others + n_col - 1 + ups + downs)

    def give(j):
        return pltpu.make_async_remote_copy(
            src_ref=pk_ref.at[j],
            dst_ref=got_ref.at[d],
            send_sem=asend_sem.at[j],
            recv_sem=arecv_sem.at[d],
            device_id={"row": peer(j)},
            device_id_type=MESH,
        )

    def relay(j, o):
        w = peer(j)
        return pltpu.make_async_remote_copy(
            src_ref=got_ref.at[w],
            dst_ref=got_ref.at[w],
            send_sem=rsend_sem.at[o - 1, j],
            recv_sem=arecv_sem.at[w],
            device_id={"col": lax.rem(z + o, n_col)},
            device_id_type=MESH,
        )

    def incoming(w):
        return pltpu.make_async_remote_copy(
            src_ref=got_ref.at[w],
            dst_ref=got_ref.at[w],
            send_sem=rsend_sem.at[0, 0],
            recv_sem=arecv_sem.at[w],
            device_id={"col": lax.rem(z + 1, n_col)},
            device_id_type=MESH,
        )

    def pass_on(j, cond=True):
        @pl.when((peer(j) != d) & cond)
        def _():
            incoming(peer(j)).wait_recv()
            for o in range(1, n_col):
                relay(j, o).start()

    def need(w, cond=True):
        @pl.when((w != d) & (lax.rem(w + d, n_col) != z) & cond)
        def _():
            incoming(w).wait_recv()

    def forward(r):
        return pltpu.make_async_remote_copy(
            src_ref=got_ref.at[2 * r + 1],
            dst_ref=fw_ref.at[r],
            send_sem=fsend_sem.at[r],
            recv_sem=frecv_sem.at[r],
            device_id={"row": d + 1},
            device_id_type=MESH,
        )

    def send_on(r, cond=True):
        need(2 * r + 1, cond)

        @pl.when(has_dn & cond)
        def _():
            forward(r).start()

    def arrive(r, cond=True):
        @pl.when(has_up & cond)
        def _():
            forward(r).wait_recv()

    def link(k, p, c):
        return pltpu.make_async_remote_copy(
            src_ref=cs_ref.at[p, c, k],
            dst_ref=cr_ref.at[p, c, k],
            send_sem=send_sem.at[k, p, c],
            recv_sem=recv_sem.at[k, p, c],
            device_id={"row": across[k]},
            device_id_type=MESH,
        )

    def launch(k, p, c):
        only(has_edge[k], lambda: link(k, p, c).start())

    def land(k, p, c):
        only(has_edge[k], lambda: link(k, p, c).wait())

    def swap(k, r):
        return pltpu.make_async_remote_copy(
            src_ref=hsend_ref.at[r, k],
            dst_ref=hrecv_ref.at[r, k],
            send_sem=hsend_sem.at[k, r],
            recv_sem=hrecv_sem.at[k, r],
            device_id={"row": across[k]},
            device_id_type=MESH,
        )

    lane = lax.broadcasted_iota(jnp.int32, (nb, block_rows), 1)
    lane_h = lax.broadcasted_iota(jnp.int32, (nb, half), 1)
    lane_q = lax.broadcasted_iota(jnp.int32, (nb // 2, half), 1)
    low, high = lane_h < nb, lane_h >= nb

    def turned(x):
        return pltpu.roll(x, nb, 1)

    def expanded(block):
        return pltpu.roll(jnp.where(lane < band, block, 0.0), 0, 1, stride=1, stride_axis=0)

    def prepare_even(r, q):
        block = got_ref[2 * r]
        vh, vl = split(expanded(block))
        on = d >= first_ref[2 * r]
        factor = jnp.where(high & on, block[:, half:], 0.0)
        th = factor.astype(BF16).astype(F32)
        tl = factor - th
        left = jnp.concatenate([th + turned(th), turned(tl)], axis=1)
        u = dot(left.astype(BF16), jnp.concatenate([vh, vl, vh, vh], axis=0))
        uh, ul = split(u)
        op = dot_tn(
            jnp.concatenate([vh, vh, vl, jnp.zeros_like(vh)], axis=0),
            jnp.concatenate([uh, ul, uh, uh], axis=0),
        )
        hi, lo = split(op)
        rh_ref[q] = hi
        rl_ref[q] = lo
        return hi, lo

    def prepare_odd(r, q, oh, ol):
        own = got_ref[2 * r + 1]
        other = fw_ref[r]
        first = first_ref[2 * r + 1]
        none = jnp.zeros((nb, half), F32)
        upper = jnp.concatenate([expanded(other)[:, half:], none], axis=1)
        lower = jnp.concatenate([none, expanded(own)[:, :half]], axis=1)
        proj = jnp.concatenate(
            [jnp.where(is_odd, lower, upper), jnp.where(is_odd, upper, lower)], axis=0
        )
        t_up = jnp.where(d - 1 >= first, other[:, half:], 0.0)
        t_dn = jnp.where((d >= first) & has_dn, own[:, half:], 0.0)
        both = jnp.concatenate(
            [
                jnp.where(low, turned(jnp.where(is_odd, t_dn, t_up)), 0.0),
                jnp.where(high, jnp.where(is_odd, t_up, t_dn), 0.0),
            ],
            axis=0,
        )
        ph, pm = split(proj)
        bh, bl = split(both)
        w = dot_tn(
            jnp.concatenate([ph, pm], axis=0), jnp.concatenate([bh, bh], axis=0)
        ) + dot_tn(ph, bl)
        wh, wl = split(w)
        ws_ref[q] = jnp.concatenate([wh, wh], axis=1)
        wl_ref[q] = wl
        s = proj - (dot(ph, oh) + (dot(pm, oh) + dot(ph, ol)))
        sh, sl = split(s)
        sh_ref[q] = sh
        sl_ref[q] = sl
        return sh, sl

    def prepare_link(q, at, sh, sl):
        b = lax.rem(q + SLOTS - 1, SLOTS)
        wh = ws_ref[b, :, pl.ds(0, half)]
        h = dot(sh, wh) + (dot(sl, wh) + dot(sh, wl_ref[b]))
        top, bottom = h[:nb], h[nb:]
        th = top.astype(BF16).astype(F32)
        hi, lo = jnp.where(high, th, 0.0), jnp.where(high, top - th, 0.0)
        ho_ref[q, 0] = jnp.concatenate([hi + turned(hi), turned(lo)], axis=1).astype(BF16)
        bh = bottom.astype(BF16).astype(F32)
        hi, lo = jnp.where(low, bh, 0.0), jnp.where(low, bottom - bh, 0.0)
        ho_ref[q, 1] = jnp.concatenate([hi + turned(hi), lo], axis=1).astype(BF16)
        hd_ref[q, pl.ds(0, nb)] = jnp.where(low, top, 0.0)
        hd_ref[q, pl.ds(nb, nb)] = jnp.where(high, bottom, 0.0)
        quarter = nb // 2
        hsend_ref[at, 0] = jnp.where(lane_q < nb, top[:quarter], turned(top[quarter:]))
        hsend_ref[at, 1] = jnp.where(lane_q < nb, turned(bottom[:quarter]), bottom[quarter:])

    def swap_start(r, cond=True):
        for k in range(2):
            have = cond if has_edge[k] is None else has_edge[k] & cond
            only(None if have is True else have, lambda k=k: swap(k, r).start())

    def diagonal(r, q):
        x, s = hrecv_ref[r, 0], hrecv_ref[r, 1]
        left, right = lane_q < nb, lane_q >= nb
        total = hd_ref[q] + jnp.concatenate(
            [
                jnp.where(left, x, 0.0),
                jnp.where(left, turned(x), 0.0),
                jnp.where(right, turned(s), 0.0),
                jnp.where(right, s, 0.0),
            ],
            axis=0,
        )
        hi, lo = split(total)
        return jnp.concatenate([hi, hi], axis=1), lo

    def prepare(r, q, at):
        sh, sl = prepare_odd(r, q, *prepare_even(r, q))
        prepare_link(q, at, sh, sl)

    def project(y, q):
        yh, yl = split(y)
        return dot(sh_ref[q], yh) + (dot(sl_ref[q], yh) + dot(sh_ref[q], yl))

    def reflect(x, q):
        xh, xl = split(x)
        return x - (dot(rh_ref[q], xh) + (dot(rl_ref[q], xh) + dot(rh_ref[q], xl)))

    def corrected(q, c):
        return y_ref[c] - (dot(ws_ref[q], st_ref[c]) + dot(wl_ref[q], st_ref[c, pl.ds(0, half)]))

    def total(k, p, c):
        at = k * nb
        th, tl = split(d_ref[c, pl.ds(at, nb)] + cr_ref[p, c, k])
        st_ref[c, pl.ds(at, nb)] = th
        st_ref[c, pl.ds(half + at, nb)] = tl
        return th, tl

    def answer(k, p, n, c):
        land(k, p, c)
        th, tl = total(k, p, c)
        cs_ref[n, c, 1 - k] = g_ref[c, pl.ds((1 - k) * nb, nb)] - dot(
            ho_ref[n, 1 - k], jnp.concatenate([th, tl, th, th], axis=0)
        )
        launch(1 - k, n, c)

    def columns(c):
        return pl.ds(c * CHUNK, CHUNK)

    def give_all():
        turn = d // n_col
        for j in range(n_peers):
            i = lax.rem(j + turn, n_peers)

            @pl.when(peer(i) != d)
            def _():
                give(i).start()

    early = d < FIRST

    @pl.when(early)
    def _():
        give_all()

    lead = min(LEAD // n_col, n_peers)
    soon = min(FIRST // n_col, lead)
    for j in range(soon):
        pass_on(j)

    @pl.when(jnp.logical_not(early))
    def _():
        give_all()

    send_on(0)
    need(0)
    ops = prepare_even(0, 0)
    arrive(0)
    prepare_odd(0, 0, *ops)
    eig_copy.wait()
    for c in range(n_chunks):
        x = project(e_ref[:, columns(c)], 0)
        d_ref[c] = x
        for k in range(2):
            cs_ref[0, c, k] = x[k * nb : (k + 1) * nb]
            launch(k, 0, c)

    for r in range(1, min(3, rounds)):
        send_on(r)
        need(2 * r)
    for c in range(n_chunks):
        y_ref[c] = reflect(e_ref[:, columns(c)], 0)
    for r in range(1, min(3, rounds)):
        arrive(r)
        prepare(r, r, r)
        swap_start(r)
    for c in range(n_chunks):
        g_ref[c] = project(y_ref[c], 1)
    for j in range(soon, lead):
        pass_on(j)
    for r in range(3, min(AHEAD, rounds)):
        send_on(r)

    def step(r, carry):
        p = lax.rem(r, SLOTS)
        n = lax.rem(r + 1, SLOTS)
        for c in range(n_chunks):
            answer(1, p, n, c)

        now = (2 * r + LEAD) // n_col
        pass_on(now, ((2 * r + 2 + LEAD) // n_col > now) & (now < n_peers))
        send_on(r + AHEAD, r + AHEAD < rounds)
        later = r + 3 < rounds
        need(2 * r + 6, later)
        arrive(r + 3, later)
        after = jnp.minimum(r + 3, rounds - 1)
        prepare(after, lax.rem(r + 3, SLOTS), r + 3)
        swap_start(r + 3, later)

        for c in range(n_chunks):
            answer(0, p, n, c)

        for k in range(2):
            only(has_edge[k], lambda k=k: swap(k, r + 1).wait())
        both, low_part = diagonal(r + 1, n)
        for c in range(n_chunks):
            y_ref[c] = reflect(corrected(p, c), n)
        for c in range(n_chunks):
            g_ref[c] = project(y_ref[c], lax.rem(r + 2, SLOTS))
        for c in range(n_chunks):
            less = dot(both, st_ref[c]) + dot(low_part, st_ref[c, pl.ds(0, half)])
            for k in range(2):
                d_ref[c, pl.ds(k * nb, nb)] = cs_ref[n, c, k] - less[k * nb : (k + 1) * nb]
        return carry

    lax.fori_loop(0, rounds - 1, step, 0)

    p = (rounds - 1) % SLOTS
    for c in range(n_chunks):
        for k in (1, 0):
            land(k, p, c)
            total(k, p, c)
        out_ref[:, columns(c)] = corrected(p, c)

    for j in range(n_peers):

        @pl.when(peer(j) != d)
        def _():
            give(j).wait_send()
            for o in range(1, n_col):
                relay(j, o).wait_send()

    @pl.when(has_dn)
    def _():
        def done(r, carry):
            forward(r).wait_send()
            return carry

        lax.fori_loop(0, rounds, done, 0)


def sweep(eigvecs, reflectors, factors, first_block, n_row, n_col):
    rows = eigvecs.shape[0]
    nb, band = reflectors.shape[2:]
    block_rows = nb + band
    windows = n_row * reflectors.shape[0]
    rounds = windows // 2
    n_chunks = MAX_LIVE // CHUNK
    n_peers = n_row // n_col
    vmem = pltpu.VMEM
    dma = pltpu.SemaphoreType.DMA
    hbm = pl.BlockSpec(memory_space=pltpu.HBM)
    return pl.pallas_call(
        functools.partial(kernel, n_row, n_col),
        out_shape=jax.ShapeDtypeStruct((rows, MAX_LIVE), F32),
        in_specs=[pl.BlockSpec(memory_space=pltpu.SMEM), hbm, hbm, hbm],
        out_specs=pl.BlockSpec(memory_space=pltpu.VMEM),
        scratch_shapes=[
            vmem((rows, MAX_LIVE), F32),
            vmem((n_peers + 1, nb, band), F32),
            vmem((n_peers + 1, nb, nb), F32),
            vmem((n_peers, nb, block_rows), F32),
            vmem((windows, nb, block_rows), F32),
            vmem((rounds, nb, block_rows), F32),
            vmem((n_chunks, rows, CHUNK), F32),
            vmem((n_chunks, 2 * nb, CHUNK), F32),
            vmem((n_chunks, 2 * nb, CHUNK), F32),
            vmem((n_chunks, 4 * nb, CHUNK), BF16),
            vmem((SLOTS, n_chunks, 2, nb, CHUNK), F32),
            vmem((SLOTS, n_chunks, 2, nb, CHUNK), F32),
            vmem((rounds + 3, 2, nb // 2, 2 * nb), F32),
            vmem((rounds, 2, nb // 2, 2 * nb), F32),
            vmem((SLOTS, rows, rows), BF16),
            vmem((SLOTS, rows, rows), BF16),
            vmem((SLOTS, 2 * nb, rows), BF16),
            vmem((SLOTS, 2 * nb, rows), BF16),
            vmem((SLOTS, 2, nb, 4 * nb), BF16),
            vmem((SLOTS, 2 * nb, 2 * nb), F32),
            vmem((SLOTS, rows, 4 * nb), BF16),
            vmem((SLOTS, rows, 2 * nb), BF16),
            dma((2, n_peers + 1)),
            dma,
            dma((n_peers,)),
            dma((max(n_col - 1, 1), n_peers)),
            dma((windows,)),
            dma((2, SLOTS, n_chunks)),
            dma((2, SLOTS, n_chunks)),
            dma((rounds,)),
            dma((rounds,)),
            dma((2, rounds)),
            dma((2, rounds)),
        ],
        compiler_params=pltpu.CompilerParams(collective_id=0, has_side_effects=True),
        name="sweep",
    )(first_block, eigvecs, reflectors, factors)


def body(eigvecs, reflectors, factors, first_block, live_count):
    n_row = lax.axis_size("row")
    n_col = lax.axis_size("col")
    vectors = sweep(eigvecs, reflectors, factors, first_block, n_row, n_col)
    col_count = eigvecs.shape[1]
    vectors = jnp.pad(vectors, ((0, 0), (0, col_count - MAX_LIVE)))
    kept_mask = jnp.arange(col_count, dtype=jnp.int32) < live_count[0]
    return jnp.where(kept_mask[None, :], vectors, 0.0)


def solution(mesh):
    placed = (
        P("row", "col"),
        P("row", None, None, None),
        P("row", None, None, None),
        P(),
        P("col"),
    )
    return jax.shard_map(
        body, mesh=mesh, in_specs=placed, out_specs=P("row", "col"), check_vma=False
    )
```

```python
import functools

import jax
import jax.numpy as jnp
from jax import lax
from jax.experimental import pallas as pl
from jax.experimental.pallas import tpu as pltpu
from jax.sharding import PartitionSpec as P

MAX_LIVE = 768
CHUNK = 256
AHEAD = 4
LEAD = 16
FIRST = 8
SLOTS = 4
RING = 8
F32 = jnp.float32
BF16 = jnp.bfloat16
MESH = pl.DeviceIdType.MESH
TN = (((0,), (0,)), ((), ()))


def split(x):
    hi = x.astype(BF16)
    lo = (x - hi.astype(F32)).astype(BF16)
    return hi, lo


def dot(a, b):
    return jnp.dot(a, b, preferred_element_type=F32)


def dot_tn(a, b):
    return lax.dot_general(a, b, TN, preferred_element_type=F32)


def kernel(
    n_row,
    n_col,
    first_ref,
    eig_hbm,
    refl_hbm,
    fact_hbm,
    out_ref,
    e_ref,
    v_ref,
    t_ref,
    pk_ref,
    got_ref,
    fw_ref,
    y_ref,
    g_ref,
    d_ref,
    cs_ref,
    cr_ref,
    hsend_ref,
    hrecv_ref,
    rh_ref,
    rl_ref,
    sh_ref,
    sl_ref,
    hd_ref,
    wh_ref,
    wl_ref,
    op_ref,
    local_sem,
    eig_sem,
    asend_sem,
    rsend_sem,
    arecv_sem,
    send_sem,
    recv_sem,
    fsend_sem,
    frecv_sem,
    hsend_sem,
    hrecv_sem,
):
    d = lax.axis_index("row")
    z = lax.axis_index("col")
    windows, nb, block_rows = got_ref.shape
    band = block_rows - nb
    rounds = windows // 2
    half = block_rows // 2
    n_chunks = y_ref.shape[0]
    n_peers = n_row // n_col
    kin = lax.rem(z - d + n_row * n_col, n_col)

    odd = lax.rem(d, 2)
    is_odd = odd == 1
    has_up = d > 0
    has_dn = d < n_row - 1
    has_edge = (has_up & has_dn, None)
    across = (d - 1 + 2 * odd, d + 1 - 2 * odd)

    def only(cond, todo):
        if cond is None:
            todo()
        else:
            pl.when(cond)(todo)

    def peer(j):
        return kin + n_col * j

    barrier = pltpu.get_barrier_semaphore()

    def greet(cond, where):
        @pl.when(cond)
        def _():
            pl.semaphore_signal(barrier, inc=1, device_id=where, device_id_type=MESH)

    for j in range(n_peers):
        greet(peer(j) != d, {"row": peer(j)})
    for o in range(1, n_col):
        pl.semaphore_signal(
            barrier, inc=1, device_id={"col": lax.rem(z + o, n_col)}, device_id_type=MESH
        )
    greet(has_up, {"row": d - 1})
    greet(has_dn, {"row": d + 1})

    at, within = d // n_col, lax.rem(d, n_col)
    fetches = [
        pltpu.make_async_copy(refl_hbm.at[:, kin], v_ref.at[pl.ds(0, n_peers)], local_sem.at[0]),
        pltpu.make_async_copy(fact_hbm.at[:, kin], t_ref.at[pl.ds(0, n_peers)], local_sem.at[1]),
        pltpu.make_async_copy(refl_hbm.at[at, within], v_ref.at[n_peers], local_sem.at[2]),
        pltpu.make_async_copy(fact_hbm.at[at, within], t_ref.at[n_peers], local_sem.at[3]),
    ]
    for copy in fetches:
        copy.start()
    eig_copy = pltpu.make_async_copy(
        eig_hbm.at[:, pl.ds(0, n_chunks * CHUNK)], e_ref, eig_sem
    )
    eig_copy.start()

    @pl.when(jnp.logical_not(has_up))
    def _():
        fw_ref[...] = jnp.zeros_like(fw_ref)

    @pl.when(jnp.logical_not(has_edge[0]))
    def _():
        for r in range(rounds):
            hrecv_ref[r, 0] = jnp.zeros((nb // 2, half), F32)
        for p in range(SLOTS):
            for c in range(n_chunks):
                cr_ref[p, c, 0] = jnp.zeros((nb, CHUNK), F32)

    for copy in fetches:
        copy.wait()
    for j in range(n_peers + 1):
        packed = jnp.concatenate([v_ref[j], t_ref[j]], axis=1)
        if j < n_peers:
            pk_ref[j] = packed
        else:
            got_ref[d] = packed

    ups = (d + n_row - 1) // n_row
    downs = (2 * n_row - 2 - d) // n_row
    others = (lax.rem(2 * d - z + n_row * n_col, n_col) + n_col - 1) // n_col
    pl.semaphore_wait(barrier, n_peers - 1 + others + n_col - 1 + ups + downs)

    def give(j):
        return pltpu.make_async_remote_copy(
            src_ref=pk_ref.at[j],
            dst_ref=got_ref.at[d],
            send_sem=asend_sem,
            recv_sem=arecv_sem.at[d],
            device_id={"row": peer(j)},
            device_id_type=MESH,
        )

    def relay(j, o):
        w = peer(j)
        return pltpu.make_async_remote_copy(
            src_ref=got_ref.at[w],
            dst_ref=got_ref.at[w],
            send_sem=rsend_sem,
            recv_sem=arecv_sem.at[w],
            device_id={"col": lax.rem(z + o, n_col)},
            device_id_type=MESH,
        )

    def incoming(w):
        return pltpu.make_async_remote_copy(
            src_ref=got_ref.at[w],
            dst_ref=got_ref.at[w],
            send_sem=rsend_sem,
            recv_sem=arecv_sem.at[w],
            device_id={"col": lax.rem(z + 1, n_col)},
            device_id_type=MESH,
        )

    def pass_on(j, cond=True):
        @pl.when((peer(j) != d) & cond)
        def _():
            incoming(peer(j)).wait_recv()
            for o in range(1, n_col):
                relay(j, o).start()

    def need(w, cond=True):
        @pl.when((w != d) & (lax.rem(w + d, n_col) != z) & cond)
        def _():
            incoming(w).wait_recv()

    def forward(r):
        return pltpu.make_async_remote_copy(
            src_ref=got_ref.at[2 * r + 1],
            dst_ref=fw_ref.at[r],
            send_sem=fsend_sem,
            recv_sem=frecv_sem.at[lax.rem(r, RING)],
            device_id={"row": d + 1},
            device_id_type=MESH,
        )

    def send_on(r, cond=True):
        need(2 * r + 1, cond)

        @pl.when(has_dn & cond)
        def _():
            forward(r).start()

    def arrive(r, cond=True):
        @pl.when(has_up & cond)
        def _():
            forward(r).wait_recv()

    def link(k, p, c):
        return pltpu.make_async_remote_copy(
            src_ref=cs_ref.at[p, c, k],
            dst_ref=cr_ref.at[p, c, k],
            send_sem=send_sem.at[k, p, c],
            recv_sem=recv_sem.at[k, p, c],
            device_id={"row": across[k]},
            device_id_type=MESH,
        )

    def launch(k, p, c):
        only(has_edge[k], lambda: link(k, p, c).start())

    def land(k, p, c):
        only(has_edge[k], lambda: link(k, p, c).wait())

    def swap(k, r):
        return pltpu.make_async_remote_copy(
            src_ref=hsend_ref.at[r, k],
            dst_ref=hrecv_ref.at[r, k],
            send_sem=hsend_sem.at[k],
            recv_sem=hrecv_sem.at[k, lax.rem(r, RING)],
            device_id={"row": across[k]},
            device_id_type=MESH,
        )

    lane = lax.broadcasted_iota(jnp.int32, (nb, block_rows), 1)
    lane_h = lax.broadcasted_iota(jnp.int32, (nb, half), 1)
    lane_q = lax.broadcasted_iota(jnp.int32, (nb // 2, half), 1)
    low, high = lane_h < nb, lane_h >= nb
    wide = lax.broadcasted_iota(jnp.int32, (half, half), 1) < nb

    def turned(x):
        return pltpu.roll(x, nb, 1)

    def expanded(block):
        return pltpu.roll(jnp.where(lane < band, block, 0.0), 0, 1, stride=1, stride_axis=0)

    def prepare_even(r, q):
        block = got_ref[2 * r]
        vh, vl = split(expanded(block))
        on = d >= first_ref[2 * r]
        factor = jnp.where(high & on, block[:, half:], 0.0)
        th = factor.astype(BF16).astype(F32)
        tl = factor - th
        left = jnp.concatenate([th + turned(th), turned(tl)], axis=1)
        u = dot(left.astype(BF16), jnp.concatenate([vh, vl, vh, vh], axis=0))
        uh, ul = split(u)
        op = dot_tn(
            jnp.concatenate([vh, vh, vl, jnp.zeros_like(vh)], axis=0),
            jnp.concatenate([uh, ul, uh, uh], axis=0),
        )
        hi, lo = split(op)
        rh_ref[q] = hi
        rl_ref[q] = lo
        return hi, lo

    def stacked(x):
        hi = x.astype(BF16)
        lo = jnp.where(low, x - hi.astype(F32), 0.0).astype(BF16)
        return jnp.concatenate([hi, lo], axis=1)

    def prepare_odd(r, q, oh, ol):
        own = got_ref[2 * r + 1]
        other = fw_ref[r]
        first = first_ref[2 * r + 1]
        none = jnp.zeros((nb, half), F32)
        up, dn = expanded(other)[:, half:], expanded(own)[:, :half]
        t_up = jnp.where(high & (d - 1 >= first), other[:, half:], 0.0)
        t_dn = jnp.where(high & (d >= first) & has_dn, own[:, half:], 0.0)
        rows = []
        for k in range(2):
            flip = is_odd if k == 0 else jnp.logical_not(is_odd)
            part = jnp.where(flip, dn, up)
            rows.append(
                jnp.concatenate(
                    [jnp.where(flip, none, part), jnp.where(flip, part, none)], axis=1
                )
            )
            factor = jnp.where(flip, t_dn, t_up)
            ph, pm = split(part)
            fh, fm = split(factor + turned(factor))
            w = dot_tn(
                jnp.concatenate([ph, ph, pm, jnp.zeros_like(ph)], axis=0),
                jnp.concatenate([fh, fm, fh, fh], axis=0),
            )
            wh, wl = split(w)
            wh_ref[q, k] = wh
            wl_ref[q, k] = wl
            op_ref[q, k, pl.ds(half, half)] = jnp.concatenate(
                [wh, jnp.where(wide, wl.astype(F32), 0.0).astype(BF16)], axis=1
            )
        proj = jnp.concatenate(rows, axis=0)
        ph, pm = split(proj)
        s = proj - (dot(ph, oh) + (dot(pm, oh) + dot(ph, ol)))
        sh, sl = split(s)
        sh_ref[q] = sh
        sl_ref[q] = sl
        return sh, sl

    def prepare_link(q, at, sh, sl):
        b = lax.rem(q + SLOTS - 1, SLOTS)
        quarter = nb // 2
        for k in range(2):
            flip = is_odd if k == 0 else jnp.logical_not(is_odd)
            ah = jnp.where(flip, sh[:, half:].astype(F32), sh[:, :half].astype(F32)).astype(BF16)
            al = jnp.where(flip, sl[:, half:].astype(F32), sl[:, :half].astype(F32)).astype(BF16)
            wh = wh_ref[b, k]
            h = dot(
                jnp.concatenate([ah, al], axis=1), jnp.concatenate([wh, wh], axis=0)
            ) + dot(ah, wl_ref[b, k])
            here, there = h[k * nb : (k + 1) * nb], h[(1 - k) * nb : (2 - k) * nb]
            op_ref[b, k, pl.ds(0, nb)] = stacked(there)
            hd_ref[q, k] = here
            hsend_ref[at, k] = jnp.where(lane_q < nb, here[:quarter], here[quarter:])

    def swap_start(r, cond=True):
        for k in range(2):
            have = cond if has_edge[k] is None else has_edge[k] & cond
            only(None if have is True else have, lambda k=k: swap(k, r).start())

    def combine(r, q, cond=True):
        b = lax.rem(q + SLOTS - 1, SLOTS)
        for k in range(2):
            have = cond if has_edge[k] is None else has_edge[k] & cond
            only(None if have is True else have, lambda k=k: swap(k, r).wait_recv())
        for k in range(2):
            x = hrecv_ref[r, k]
            left = lane_q < nb
            theirs = jnp.concatenate(
                [jnp.where(left, x, turned(x)), jnp.where(left, turned(x), x)], axis=0
            )
            op_ref[b, k, pl.ds(nb, nb)] = stacked(hd_ref[q, k] + theirs)

    def prepare(r, q, at):
        sh, sl = prepare_odd(r, q, *prepare_even(r, q))
        prepare_link(q, at, sh, sl)

    def project(y, q):
        yh, yl = split(y)
        return dot(sh_ref[q], yh) + (dot(sl_ref[q], yh) + dot(sh_ref[q], yl))

    def reflect(x, q):
        xh, xl = split(x)
        return x - (dot(rh_ref[q], xh) + (dot(rl_ref[q], xh) + dot(rh_ref[q], xl)))

    def total(k, p, c):
        th, tl = split(d_ref[c, k] + cr_ref[p, c, k])
        return jnp.concatenate([th, tl, th, th], axis=0)

    def side(k):
        h = odd if k == 0 else 1 - odd
        return pl.ds(pl.multiple_of(h * half, half), half)

    def answer(k, p, n, c):
        res = dot(op_ref[p, k], total(k, p, c))
        x = g_ref[c, 1 - k] - res[:nb]
        cs_ref[n, c, 1 - k] = x
        launch(1 - k, n, c)
        y_ref[c, side(k)] = y_ref[c, side(k)] - res[half:]
        if k == 1:
            d_ref[c, 1] = res[nb:half]
        else:
            d_ref[c, 1] = x - d_ref[c, 1]
            d_ref[c, 0] = cs_ref[n, c, 0] - res[nb:half]

    def columns(c):
        return pl.ds(c * CHUNK, CHUNK)

    def give_all():
        turn = d // n_col
        for j in range(n_peers):
            i = lax.rem(j + turn, n_peers)

            @pl.when(peer(i) != d)
            def _():
                give(i).start()

    give_all()
    lead = min(LEAD // n_col, n_peers)
    soon = min(FIRST // n_col, lead)
    for j in range(soon):
        pass_on(j)

    send_on(0)
    need(0)
    ops = prepare_even(0, 0)
    send_on(1)
    arrive(0)
    prepare_odd(0, 0, *ops)
    eig_copy.wait()
    for c in range(n_chunks):
        x = project(e_ref[:, columns(c)], 0)
        for k in range(2):
            part = x[k * nb : (k + 1) * nb]
            d_ref[c, k] = part
            cs_ref[0, c, k] = part
            launch(k, 0, c)

    for j in range(soon, lead):
        pass_on(j)
    for c in range(n_chunks):
        y_ref[c] = reflect(e_ref[:, columns(c)], 0)
    for r in range(1, min(3, rounds)):
        if r > 1:
            send_on(r)
        need(2 * r)
        arrive(r)
        prepare(r, r, r)
        swap_start(r)
        if r == 1:
            for c in range(n_chunks):
                x = project(y_ref[c], 1)
                g_ref[c, 0] = x[:nb]
                g_ref[c, 1] = x[nb:]
    for r in range(3, min(AHEAD, rounds)):
        send_on(r)
    combine(1, 1)

    def step(r, carry):
        p = lax.rem(r, SLOTS)
        n = lax.rem(r + 1, SLOTS)
        for c in range(n_chunks):
            land(1, p, c)
        for c in range(n_chunks):
            answer(1, p, n, c)

        now = (2 * r + LEAD) // n_col
        pass_on(now, ((2 * r + 2 + LEAD) // n_col > now) & (now < n_peers))
        send_on(r + AHEAD, r + AHEAD < rounds)
        later = r + 3 < rounds
        need(2 * r + 6, later)
        arrive(r + 3, later)
        after = jnp.minimum(r + 3, rounds - 1)
        prepare(after, lax.rem(r + 3, SLOTS), r + 3)
        swap_start(r + 3, later)

        for c in range(n_chunks):
            land(0, p, c)
            answer(0, p, n, c)

        for c in range(n_chunks):
            y_ref[c] = reflect(y_ref[c], n)
        q = lax.rem(r + 2, SLOTS)
        for c in range(n_chunks):
            x = project(y_ref[c], q)
            g_ref[c, 0] = x[:nb]
            g_ref[c, 1] = x[nb:]
        combine(jnp.minimum(r + 2, rounds - 1), q, r + 2 < rounds)
        return carry

    lax.fori_loop(0, rounds - 1, step, 0)

    p = (rounds - 1) % SLOTS
    for k in (1, 0):
        for c in range(n_chunks):
            land(k, p, c)
            out_ref[side(k), columns(c)] = y_ref[c, side(k)] - dot(
                op_ref[p, k, pl.ds(half, half)], total(k, p, c)
            )

    def sent(sem, src, dst):
        pltpu.make_async_remote_copy(
            src_ref=src,
            dst_ref=dst,
            send_sem=sem,
            recv_sem=frecv_sem.at[0],
            device_id={"row": d},
            device_id_type=MESH,
        ).wait_send()

    def gone(count):
        blocks = pl.ds(0, count)
        sent(asend_sem, pk_ref.at[blocks], got_ref.at[blocks])
        if n_col > 1:
            blocks = pl.ds(0, count * (n_col - 1))
            sent(rsend_sem, got_ref.at[blocks], got_ref.at[blocks])

    @pl.when(others > 0)
    def _():
        gone(n_peers)

    @pl.when(others == 0)
    def _():
        gone(n_peers - 1)

    @pl.when(has_dn)
    def _():
        sent(fsend_sem, got_ref.at[pl.ds(0, rounds)], fw_ref)

    for k in range(2):
        blocks = pl.ds(0, rounds - 1)
        only(
            has_edge[k],
            lambda k=k: sent(
                hsend_sem.at[k], hsend_ref.at[blocks, k], hrecv_ref.at[blocks, k]
            ),
        )


def sweep(eigvecs, reflectors, factors, first_block, n_row, n_col):
    rows = eigvecs.shape[0]
    nb, band = reflectors.shape[2:]
    block_rows = nb + band
    windows = n_row * reflectors.shape[0]
    rounds = windows // 2
    n_chunks = MAX_LIVE // CHUNK
    n_peers = n_row // n_col
    reflectors = reflectors.reshape(n_peers, n_col, nb, band)
    factors = factors.reshape(n_peers, n_col, nb, nb)
    vmem = pltpu.VMEM
    dma = pltpu.SemaphoreType.DMA
    hbm = pl.BlockSpec(memory_space=pltpu.HBM)
    return pl.pallas_call(
        functools.partial(kernel, n_row, n_col),
        out_shape=jax.ShapeDtypeStruct((rows, MAX_LIVE), F32),
        in_specs=[pl.BlockSpec(memory_space=pltpu.SMEM), hbm, hbm, hbm],
        out_specs=pl.BlockSpec(memory_space=pltpu.VMEM),
        scratch_shapes=[
            vmem((rows, MAX_LIVE), F32),
            vmem((n_peers + 1, nb, band), F32),
            vmem((n_peers + 1, nb, nb), F32),
            vmem((n_peers, nb, block_rows), F32),
            vmem((windows, nb, block_rows), F32),
            vmem((rounds, nb, block_rows), F32),
            vmem((n_chunks, rows, CHUNK), F32),
            vmem((n_chunks, 2, nb, CHUNK), F32),
            vmem((n_chunks, 2, nb, CHUNK), F32),
            vmem((SLOTS, n_chunks, 2, nb, CHUNK), F32),
            vmem((SLOTS, n_chunks, 2, nb, CHUNK), F32),
            vmem((rounds + 3, 2, nb // 2, 2 * nb), F32),
            vmem((rounds, 2, nb // 2, 2 * nb), F32),
            vmem((SLOTS, rows, rows), BF16),
            vmem((SLOTS, rows, rows), BF16),
            vmem((SLOTS, 2 * nb, rows), BF16),
            vmem((SLOTS, 2 * nb, rows), BF16),
            vmem((SLOTS, 2, nb, 2 * nb), F32),
            vmem((SLOTS, 2, rows // 2, 2 * nb), BF16),
            vmem((SLOTS, 2, rows // 2, 2 * nb), BF16),
            vmem((SLOTS, 2, rows, 4 * nb), BF16),
            dma((4,)),
            dma,
            dma,
            dma,
            dma((windows,)),
            dma((2, SLOTS, n_chunks)),
            dma((2, SLOTS, n_chunks)),
            dma,
            dma((RING,)),
            dma((2,)),
            dma((2, RING)),
        ],
        compiler_params=pltpu.CompilerParams(
            collective_id=0, has_side_effects=True, vmem_limit_bytes=53 * 2**20
        ),
        name="sweep",
    )(first_block, eigvecs, reflectors, factors)


def body(eigvecs, reflectors, factors, first_block, live_count):
    n_row = lax.axis_size("row")
    n_col = lax.axis_size("col")
    vectors = sweep(eigvecs, reflectors, factors, first_block, n_row, n_col)
    col_count = eigvecs.shape[1]
    vectors = jnp.pad(vectors, ((0, 0), (0, col_count - MAX_LIVE)))
    kept_mask = jnp.arange(col_count, dtype=jnp.int32) < live_count[0]
    return jnp.where(kept_mask[None, :], vectors, 0.0)


def solution(mesh):
    placed = (
        P("row", "col"),
        P("row", None, None, None),
        P("row", None, None, None),
        P(),
        P("col"),
    )
    return jax.shard_map(
        body, mesh=mesh, in_specs=placed, out_specs=P("row", "col"), check_vma=False
    )
```

```python
import functools

import jax
import jax.numpy as jnp
from jax import lax
from jax.experimental import pallas as pl
from jax.experimental.pallas import tpu as pltpu
from jax.sharding import PartitionSpec as P

MAX_LIVE = 768
CHUNK = 256
AHEAD = 4
LEAD = 16
FIRST = 8
SLOTS = 4
RING = 8
F32 = jnp.float32
BF16 = jnp.bfloat16
MESH = pl.DeviceIdType.MESH
TN = (((0,), (0,)), ((), ()))


def split(x):
    hi = x.astype(BF16)
    lo = (x - hi.astype(F32)).astype(BF16)
    return hi, lo


def dot(a, b):
    return jnp.dot(a, b, preferred_element_type=F32)


def dot_tn(a, b):
    return lax.dot_general(a, b, TN, preferred_element_type=F32)


def kernel(
    n_row,
    n_col,
    first_ref,
    eig_hbm,
    refl_hbm,
    fact_hbm,
    out_ref,
    e_ref,
    v_ref,
    t_ref,
    pk_ref,
    got_ref,
    fw_ref,
    y_ref,
    g_ref,
    d_ref,
    cs_ref,
    cr_ref,
    hsend_ref,
    hrecv_ref,
    rh_ref,
    rl_ref,
    sh_ref,
    sl_ref,
    hd_ref,
    wh_ref,
    wl_ref,
    op_ref,
    local_sem,
    eig_sem,
    asend_sem,
    rsend_sem,
    arecv_sem,
    send_sem,
    recv_sem,
    fsend_sem,
    frecv_sem,
    hsend_sem,
    hrecv_sem,
):
    d = lax.axis_index("row")
    z = lax.axis_index("col")
    windows, nb, block_rows = got_ref.shape
    band = block_rows - nb
    rounds = windows // 2
    half = block_rows // 2
    n_chunks = y_ref.shape[0]
    n_peers = n_row // n_col
    kin = lax.rem(z - d + n_row * n_col, n_col)

    odd = lax.rem(d, 2)
    is_odd = odd == 1
    has_up = d > 0
    has_dn = d < n_row - 1
    has_edge = (has_up & has_dn, None)
    across = (d - 1 + 2 * odd, d + 1 - 2 * odd)

    def only(cond, todo):
        if cond is None:
            todo()
        else:
            pl.when(cond)(todo)

    def peer(j):
        return kin + n_col * j

    barrier = pltpu.get_barrier_semaphore()

    def greet(cond, where):
        @pl.when(cond)
        def _():
            pl.semaphore_signal(barrier, inc=1, device_id=where, device_id_type=MESH)

    for j in range(n_peers):
        greet(peer(j) != d, {"row": peer(j)})
    for o in range(1, n_col):
        pl.semaphore_signal(
            barrier, inc=1, device_id={"col": lax.rem(z + o, n_col)}, device_id_type=MESH
        )
    greet(has_up, {"row": d - 1})
    greet(has_dn, {"row": d + 1})

    at, within = d // n_col, lax.rem(d, n_col)
    fetches = [
        pltpu.make_async_copy(refl_hbm.at[:, kin], v_ref.at[pl.ds(0, n_peers)], local_sem.at[0]),
        pltpu.make_async_copy(fact_hbm.at[:, kin], t_ref.at[pl.ds(0, n_peers)], local_sem.at[1]),
        pltpu.make_async_copy(refl_hbm.at[at, within], v_ref.at[n_peers], local_sem.at[2]),
        pltpu.make_async_copy(fact_hbm.at[at, within], t_ref.at[n_peers], local_sem.at[3]),
    ]
    for copy in fetches:
        copy.start()
    eig_copy = pltpu.make_async_copy(
        eig_hbm.at[:, pl.ds(0, n_chunks * CHUNK)], e_ref, eig_sem
    )
    eig_copy.start()

    @pl.when(jnp.logical_not(has_up))
    def _():
        fw_ref[...] = jnp.zeros_like(fw_ref)

    @pl.when(jnp.logical_not(has_edge[0]))
    def _():
        for r in range(rounds):
            hrecv_ref[r, 0] = jnp.zeros((nb // 2, half), F32)
        for p in range(SLOTS):
            for c in range(n_chunks):
                cr_ref[p, c, 0] = jnp.zeros((nb, CHUNK), F32)

    for copy in fetches:
        copy.wait()
    for j in range(n_peers + 1):
        packed = jnp.concatenate([v_ref[j], t_ref[j]], axis=1)
        if j < n_peers:
            pk_ref[j] = packed
        else:
            got_ref[d] = packed

    ups = (d + n_row - 1) // n_row
    downs = (2 * n_row - 2 - d) // n_row
    others = (lax.rem(2 * d - z + n_row * n_col, n_col) + n_col - 1) // n_col
    pl.semaphore_wait(barrier, n_peers - 1 + others + n_col - 1 + ups + downs)

    def give(j):
        return pltpu.make_async_remote_copy(
            src_ref=pk_ref.at[j],
            dst_ref=got_ref.at[d],
            send_sem=asend_sem,
            recv_sem=arecv_sem.at[d],
            device_id={"row": peer(j)},
            device_id_type=MESH,
        )

    def relay(j, o):
        w = peer(j)
        return pltpu.make_async_remote_copy(
            src_ref=got_ref.at[w],
            dst_ref=got_ref.at[w],
            send_sem=rsend_sem,
            recv_sem=arecv_sem.at[w],
            device_id={"col": lax.rem(z + o, n_col)},
            device_id_type=MESH,
        )

    def incoming(w):
        return pltpu.make_async_remote_copy(
            src_ref=got_ref.at[w],
            dst_ref=got_ref.at[w],
            send_sem=rsend_sem,
            recv_sem=arecv_sem.at[w],
            device_id={"col": lax.rem(z + 1, n_col)},
            device_id_type=MESH,
        )

    def pass_on(j, cond=True):
        @pl.when((peer(j) != d) & cond)
        def _():
            incoming(peer(j)).wait_recv()
            for o in range(1, n_col):
                relay(j, o).start()

    def need(w, cond=True):
        @pl.when((w != d) & (lax.rem(w + d, n_col) != z) & cond)
        def _():
            incoming(w).wait_recv()

    def forward(r):
        return pltpu.make_async_remote_copy(
            src_ref=got_ref.at[2 * r + 1],
            dst_ref=fw_ref.at[r],
            send_sem=fsend_sem,
            recv_sem=frecv_sem.at[lax.rem(r, RING)],
            device_id={"row": d + 1},
            device_id_type=MESH,
        )

    def send_on(r, cond=True):
        need(2 * r + 1, cond)

        @pl.when(has_dn & cond)
        def _():
            forward(r).start()

    def arrive(r, cond=True):
        @pl.when(has_up & cond)
        def _():
            forward(r).wait_recv()

    def link(k, p, c):
        return pltpu.make_async_remote_copy(
            src_ref=cs_ref.at[p, c, k],
            dst_ref=cr_ref.at[p, c, k],
            send_sem=send_sem.at[k, p, c],
            recv_sem=recv_sem.at[k, p, c],
            device_id={"row": across[k]},
            device_id_type=MESH,
        )

    def launch(k, p, c):
        only(has_edge[k], lambda: link(k, p, c).start())

    def land(k, p, c):
        only(has_edge[k], lambda: link(k, p, c).wait())

    def swap(k, r):
        return pltpu.make_async_remote_copy(
            src_ref=hsend_ref.at[r, k],
            dst_ref=hrecv_ref.at[r, k],
            send_sem=hsend_sem.at[k],
            recv_sem=hrecv_sem.at[k, lax.rem(r, RING)],
            device_id={"row": across[k]},
            device_id_type=MESH,
        )

    lane = lax.broadcasted_iota(jnp.int32, (nb, block_rows), 1)
    lane_h = lax.broadcasted_iota(jnp.int32, (nb, half), 1)
    lane_q = lax.broadcasted_iota(jnp.int32, (nb // 2, half), 1)
    low, high = lane_h < nb, lane_h >= nb
    wide = lax.broadcasted_iota(jnp.int32, (half, half), 1) < nb

    def turned(x):
        return pltpu.roll(x, nb, 1)

    def expanded(block):
        return pltpu.roll(jnp.where(lane < band, block, 0.0), 0, 1, stride=1, stride_axis=0)

    def prepare_even(r, q):
        block = got_ref[2 * r]
        vh, vl = split(expanded(block))
        on = d >= first_ref[2 * r]
        factor = jnp.where(high & on, block[:, half:], 0.0)
        th = factor.astype(BF16).astype(F32)
        tl = factor - th
        left = jnp.concatenate([th + turned(th), turned(tl)], axis=1)
        u = dot(left.astype(BF16), jnp.concatenate([vh, vl, vh, vh], axis=0))
        uh, ul = split(u)
        op = dot_tn(
            jnp.concatenate([vh, vh, vl, jnp.zeros_like(vh)], axis=0),
            jnp.concatenate([uh, ul, uh, uh], axis=0),
        )
        hi, lo = split(op)
        rh_ref[q] = hi
        rl_ref[q] = lo
        return hi, lo

    def stacked(x):
        hi = x.astype(BF16)
        lo = jnp.where(low, x - hi.astype(F32), 0.0).astype(BF16)
        return jnp.concatenate([hi, lo], axis=1)

    def prepare_odd(r, q, oh, ol):
        own = got_ref[2 * r + 1]
        other = fw_ref[r]
        first = first_ref[2 * r + 1]
        none = jnp.zeros((nb, half), F32)
        up, dn = expanded(other)[:, half:], expanded(own)[:, :half]
        t_up = jnp.where(high & (d - 1 >= first), other[:, half:], 0.0)
        t_dn = jnp.where(high & (d >= first) & has_dn, own[:, half:], 0.0)
        rows = []
        for k in range(2):
            flip = is_odd if k == 0 else jnp.logical_not(is_odd)
            part = jnp.where(flip, dn, up)
            rows.append(
                jnp.concatenate(
                    [jnp.where(flip, none, part), jnp.where(flip, part, none)], axis=1
                )
            )
            factor = jnp.where(flip, t_dn, t_up)
            ph, pm = split(part)
            fh, fm = split(factor + turned(factor))
            w = dot_tn(
                jnp.concatenate([ph, ph, pm, jnp.zeros_like(ph)], axis=0),
                jnp.concatenate([fh, fm, fh, fh], axis=0),
            )
            wh, wl = split(w)
            wh_ref[q, k] = wh
            wl_ref[q, k] = wl
            op_ref[q, k, pl.ds(half, half)] = jnp.concatenate(
                [wh, jnp.where(wide, wl.astype(F32), 0.0).astype(BF16)], axis=1
            )
        proj = jnp.concatenate(rows, axis=0)
        ph, pm = split(proj)
        s = proj - (dot(ph, oh) + (dot(pm, oh) + dot(ph, ol)))
        sh, sl = split(s)
        sh_ref[q] = sh
        sl_ref[q] = sl
        return sh, sl

    def prepare_link(q, at, sh, sl):
        b = lax.rem(q + SLOTS - 1, SLOTS)
        quarter = nb // 2
        for k in range(2):
            flip = is_odd if k == 0 else jnp.logical_not(is_odd)
            ah = jnp.where(flip, sh[:, half:].astype(F32), sh[:, :half].astype(F32)).astype(BF16)
            al = jnp.where(flip, sl[:, half:].astype(F32), sl[:, :half].astype(F32)).astype(BF16)
            wh = wh_ref[b, k]
            h = dot(
                jnp.concatenate([ah, al], axis=1), jnp.concatenate([wh, wh], axis=0)
            ) + dot(ah, wl_ref[b, k])
            here, there = h[k * nb : (k + 1) * nb], h[(1 - k) * nb : (2 - k) * nb]
            op_ref[b, k, pl.ds(0, nb)] = stacked(there)
            hd_ref[q, k] = here
            hsend_ref[at, k] = jnp.where(lane_q < nb, here[:quarter], here[quarter:])

    def swap_start(r, cond=True):
        for k in range(2):
            have = cond if has_edge[k] is None else has_edge[k] & cond
            only(None if have is True else have, lambda k=k: swap(k, r).start())

    def combine(r, q, cond=True):
        b = lax.rem(q + SLOTS - 1, SLOTS)
        for k in range(2):
            have = cond if has_edge[k] is None else has_edge[k] & cond
            only(None if have is True else have, lambda k=k: swap(k, r).wait_recv())
        for k in range(2):
            x = hrecv_ref[r, k]
            left = lane_q < nb
            theirs = jnp.concatenate(
                [jnp.where(left, x, turned(x)), jnp.where(left, turned(x), x)], axis=0
            )
            op_ref[b, k, pl.ds(nb, nb)] = stacked(hd_ref[q, k] + theirs)

    def prepare(r, q, at):
        sh, sl = prepare_odd(r, q, *prepare_even(r, q))
        prepare_link(q, at, sh, sl)

    def project(y, q):
        yh, yl = split(y)
        return dot(sh_ref[q], yh) + (dot(sl_ref[q], yh) + dot(sh_ref[q], yl))

    def reflect(x, q):
        xh, xl = split(x)
        return x - (dot(rh_ref[q], xh) + (dot(rl_ref[q], xh) + dot(rh_ref[q], xl)))

    def total(k, p, c):
        th, tl = split(d_ref[c, k] + cr_ref[p, c, k])
        return jnp.concatenate([th, tl, th, th], axis=0)

    def side(k):
        h = odd if k == 0 else 1 - odd
        return pl.ds(pl.multiple_of(h * half, half), half)

    def answer(k, p, n, c):
        res = dot(op_ref[p, k], total(k, p, c))
        x = g_ref[c, 1 - k] - res[:nb]
        cs_ref[n, c, 1 - k] = x
        launch(1 - k, n, c)
        y_ref[c, side(k)] = y_ref[c, side(k)] - res[half:]
        if k == 1:
            d_ref[c, 1] = res[nb:half]
        else:
            d_ref[c, 1] = x - d_ref[c, 1]
            d_ref[c, 0] = cs_ref[n, c, 0] - res[nb:half]

    def columns(c):
        return pl.ds(c * CHUNK, CHUNK)

    def give_all():
        turn = d // n_col
        for j in range(n_peers):
            i = lax.rem(j + turn, n_peers)

            @pl.when(peer(i) != d)
            def _():
                give(i).start()

    early = d < FIRST

    @pl.when(early)
    def _():
        give_all()

    lead = min(LEAD // n_col, n_peers)
    soon = min(FIRST // n_col, lead)
    pass_on(0)

    @pl.when(jnp.logical_not(early))
    def _():
        give_all()

    for j in range(1, soon):
        pass_on(j)

    send_on(0)
    need(0)
    ops = prepare_even(0, 0)
    send_on(1)
    arrive(0)
    prepare_odd(0, 0, *ops)
    eig_copy.wait()
    for c in range(n_chunks):
        x = project(e_ref[:, columns(c)], 0)
        for k in range(2):
            part = x[k * nb : (k + 1) * nb]
            d_ref[c, k] = part
            cs_ref[0, c, k] = part
            launch(k, 0, c)

    for r in range(2, min(AHEAD, rounds)):
        send_on(r)
    for j in range(soon, lead):
        pass_on(j)
    for c in range(n_chunks):
        y_ref[c] = reflect(e_ref[:, columns(c)], 0)
    for r in range(1, min(3, rounds)):
        need(2 * r)
        arrive(r)
        prepare(r, r, r)
        swap_start(r)
        if r == 1:
            for c in range(n_chunks):
                x = project(y_ref[c], 1)
                g_ref[c, 0] = x[:nb]
                g_ref[c, 1] = x[nb:]
    combine(1, 1)

    def step(r, carry):
        p = lax.rem(r, SLOTS)
        n = lax.rem(r + 1, SLOTS)
        for c in range(n_chunks):
            land(1, p, c)
        for c in range(n_chunks):
            answer(1, p, n, c)

        now = (2 * r + LEAD) // n_col
        pass_on(now, ((2 * r + 2 + LEAD) // n_col > now) & (now < n_peers))
        send_on(r + AHEAD, r + AHEAD < rounds)
        later = r + 3 < rounds
        need(2 * r + 6, later)
        arrive(r + 3, later)
        after = jnp.minimum(r + 3, rounds - 1)
        prepare(after, lax.rem(r + 3, SLOTS), r + 3)
        swap_start(r + 3, later)

        for c in range(n_chunks):
            land(0, p, c)
            answer(0, p, n, c)

        for c in range(n_chunks):
            y_ref[c] = reflect(y_ref[c], n)
        q = lax.rem(r + 2, SLOTS)
        for c in range(n_chunks):
            x = project(y_ref[c], q)
            g_ref[c, 0] = x[:nb]
            g_ref[c, 1] = x[nb:]
        combine(jnp.minimum(r + 2, rounds - 1), q, r + 2 < rounds)
        return carry

    lax.fori_loop(0, rounds - 1, step, 0)

    p = (rounds - 1) % SLOTS
    for k in (1, 0):
        for c in range(n_chunks):
            land(k, p, c)
            out_ref[side(k), columns(c)] = y_ref[c, side(k)] - dot(
                op_ref[p, k, pl.ds(half, half)], total(k, p, c)
            )

    def sent(sem, src, dst):
        pltpu.make_async_remote_copy(
            src_ref=src,
            dst_ref=dst,
            send_sem=sem,
            recv_sem=frecv_sem.at[0],
            device_id={"row": d},
            device_id_type=MESH,
        ).wait_send()

    def gone(count):
        blocks = pl.ds(0, count)
        sent(asend_sem, pk_ref.at[blocks], got_ref.at[blocks])
        if n_col > 1:
            blocks = pl.ds(0, count * (n_col - 1))
            sent(rsend_sem, got_ref.at[blocks], got_ref.at[blocks])

    @pl.when(others > 0)
    def _():
        gone(n_peers)

    @pl.when(others == 0)
    def _():
        gone(n_peers - 1)

    @pl.when(has_dn)
    def _():
        sent(fsend_sem, got_ref.at[pl.ds(0, rounds)], fw_ref)

    for k in range(2):
        blocks = pl.ds(0, rounds - 1)
        only(
            has_edge[k],
            lambda k=k: sent(
                hsend_sem.at[k], hsend_ref.at[blocks, k], hrecv_ref.at[blocks, k]
            ),
        )


def sweep(eigvecs, reflectors, factors, first_block, n_row, n_col):
    rows = eigvecs.shape[0]
    nb, band = reflectors.shape[2:]
    block_rows = nb + band
    windows = n_row * reflectors.shape[0]
    rounds = windows // 2
    n_chunks = MAX_LIVE // CHUNK
    n_peers = n_row // n_col
    reflectors = reflectors.reshape(n_peers, n_col, nb, band)
    factors = factors.reshape(n_peers, n_col, nb, nb)
    vmem = pltpu.VMEM
    dma = pltpu.SemaphoreType.DMA
    hbm = pl.BlockSpec(memory_space=pltpu.HBM)
    return pl.pallas_call(
        functools.partial(kernel, n_row, n_col),
        out_shape=jax.ShapeDtypeStruct((rows, MAX_LIVE), F32),
        in_specs=[pl.BlockSpec(memory_space=pltpu.SMEM), hbm, hbm, hbm],
        out_specs=pl.BlockSpec(memory_space=pltpu.VMEM),
        scratch_shapes=[
            vmem((rows, MAX_LIVE), F32),
            vmem((n_peers + 1, nb, band), F32),
            vmem((n_peers + 1, nb, nb), F32),
            vmem((n_peers, nb, block_rows), F32),
            vmem((windows, nb, block_rows), F32),
            vmem((rounds, nb, block_rows), F32),
            vmem((n_chunks, rows, CHUNK), F32),
            vmem((n_chunks, 2, nb, CHUNK), F32),
            vmem((n_chunks, 2, nb, CHUNK), F32),
            vmem((SLOTS, n_chunks, 2, nb, CHUNK), F32),
            vmem((SLOTS, n_chunks, 2, nb, CHUNK), F32),
            vmem((rounds + 3, 2, nb // 2, 2 * nb), F32),
            vmem((rounds, 2, nb // 2, 2 * nb), F32),
            vmem((SLOTS, rows, rows), BF16),
            vmem((SLOTS, rows, rows), BF16),
            vmem((SLOTS, 2 * nb, rows), BF16),
            vmem((SLOTS, 2 * nb, rows), BF16),
            vmem((SLOTS, 2, nb, 2 * nb), F32),
            vmem((SLOTS, 2, rows // 2, 2 * nb), BF16),
            vmem((SLOTS, 2, rows // 2, 2 * nb), BF16),
            vmem((SLOTS, 2, rows, 4 * nb), BF16),
            dma((4,)),
            dma,
            dma,
            dma,
            dma((windows,)),
            dma((2, SLOTS, n_chunks)),
            dma((2, SLOTS, n_chunks)),
            dma,
            dma((RING,)),
            dma((2,)),
            dma((2, RING)),
        ],
        compiler_params=pltpu.CompilerParams(
            collective_id=0, has_side_effects=True, vmem_limit_bytes=53 * 2**20
        ),
        name="sweep",
    )(first_block, eigvecs, reflectors, factors)


def body(eigvecs, reflectors, factors, first_block, live_count):
    n_row = lax.axis_size("row")
    n_col = lax.axis_size("col")
    vectors = sweep(eigvecs, reflectors, factors, first_block, n_row, n_col)
    col_count = eigvecs.shape[1]
    vectors = jnp.pad(vectors, ((0, 0), (0, col_count - MAX_LIVE)))
    kept_mask = jnp.arange(col_count, dtype=jnp.int32) < live_count[0]
    return jnp.where(kept_mask[None, :], vectors, 0.0)


def solution(mesh):
    placed = (
        P("row", "col"),
        P("row", None, None, None),
        P("row", None, None, None),
        P(),
        P("col"),
    )
    return jax.shard_map(
        body, mesh=mesh, in_specs=placed, out_specs=P("row", "col"), check_vma=False
    )
```
